768 devices in a mesh: dp: 24 (over z, core), section: 4 (over x), head: 8 (over y).
Axes of the slice: x: 4, y: 8, z: 12, core: 2. Of those that a mesh axis runs over, the one named last changes fastest.
Arguments:
- q_latent: bfloat16 [4, 12288, 1536], P('section', 'dp'), may hold values from -6 to 6
- kv_latent: bfloat16 [4, 12288, 576], P('section', 'dp'), may hold values from -6 to 6
- segment_ids: int32 [12288], P('dp'), may hold values from 0 to 191, never falling along the last dimension, each value on 1 to 512 neighbouring positions
- q_weight: bfloat16 [4, 1536, 12288], P('section', 'dp', 'head'), may hold values from -100 to 100
- k_weight: bfloat16 [4, 512, 8192], P('section', None, 'head'), may hold values from -0.25 to 0.25
Outputs:
- logit_ratio: float32 [4, 64], P(None, 'head')
- scaled_q: bfloat16 [4, 1536, 12288], P('section', 'dp', 'head')
- scaled_k: bfloat16 [4, 512, 8192], P('section', None, 'head')
The draws below stay inside these ranges and needn't reach their ends.
All inputs are finite; a program needn't handle non-finite values.
Results may differ from the reference program's by a relative error of at most 0.0034.
Values may be sent and summed in bfloat16 or wider, within the bound.
No kernel may reach another device: no remote copies, remote signals or barrier semaphores. Data moves between devices by JAX's collectives and lax.ppermute only.
A program may use at most 32 MiB of HBM per device.

```python
import math
import jax
import jax.numpy as jnp
import numpy as np
from jax import lax

D_Q = 1536
D_KV = 512
NOPE = 128
ROPE = 64
HEADS = 64
SEQ = 512
LAYERS = 4
TOKENS = 12288
N_DP = 24


def draw_q_weight(key, part):
    scale_key, entry_key = jax.random.split(jax.random.fold_in(key, 11))
    head_scale = jnp.exp(jax.random.uniform(scale_key, (LAYERS, 1, HEADS, 1), jnp.float32, math.log(2.0), math.log(100.0)))
    entries = jax.random.normal(entry_key, (LAYERS, D_Q, HEADS, NOPE + ROPE), jnp.float32)
    weights = entries * head_scale / math.sqrt(D_Q)
    return weights.reshape(LAYERS, D_Q, HEADS * (NOPE + ROPE)).astype(jnp.bfloat16)


def level_of(stream_key, dims, cuts, smallest, top_value):
    def one(dim, blocks):
        steps = jax.random.uniform(jax.random.fold_in(jax.random.fold_in(stream_key, 6), dim), (blocks,), jnp.float32, smallest / len(cuts), top_value / len(cuts))
        return jnp.repeat(jnp.exp(steps), dims[dim] // blocks).reshape((-1,) + (1,) * (len(dims) - dim - 1))

    loudness = one(*cuts[0])
    for cut in cuts[1:]:
        loudness = loudness * one(*cut)
    return loudness


def split_up(amount, total, limit, slope):
    loads = [(1 << 20) // math.isqrt(standing ** slope) + 1 for standing in range(2, amount + 1)]
    rest, counts = total - limit - (amount - 1), [1] * (amount - 1)
    while rest > 0:
        free = [i for i in range(amount - 1) if counts[i] < limit]
        mass, remaining = sum([loads[i] for i in free]), rest
        for i in free:
            extra = min(limit - counts[i], max(1, remaining * loads[i] // mass), rest)
            counts[i] = counts[i] + extra
            rest = rest - extra
    return np.array([limit] + counts)


def ragged_sizes(key, amount, total, limit, skew):
    if amount == 2:
        one = jax.random.randint(key, (), max(1, total - limit), min(limit, total - 1) + 1)
        return jnp.stack([one, total - one])
    lengths = jnp.asarray(split_up(amount, total, limit, skew), jnp.int32)
    pairs = (amount - 1) // 2
    source_of, taker = lengths[1:1 + 2 * pairs:2], lengths[2:2 + 2 * pairs:2]
    margin = jnp.minimum(source_of - 1, limit - taker)
    shifted = jax.random.randint(jax.random.fold_in(key, 1), (pairs,), 0, 1 << 20) % (margin + 1)
    lengths = lengths.at[1:1 + 2 * pairs:2].set(source_of - shifted).at[2:2 + 2 * pairs:2].set(taker + shifted)
    return lengths[jax.random.permutation(jax.random.fold_in(key, 2), amount)]


def gaussian(key, extent, width, reach, cuts=(), kind=jnp.bfloat16):
    values = jax.random.normal(key, extent, jnp.float32) * width
    if len(cuts) > 0:
        values = level_of(key, extent, cuts, -0.22, 0.18) * values
    return jnp.clip(values, min=-reach, max=reach).astype(kind)


def setup_inputs(seed: int = 0) -> dict:
    arg_keys = jax.random.split(jax.random.key(seed), 6)
    return {
        "q_latent": gaussian(arg_keys[0], (LAYERS, TOKENS, D_Q), 1.0, 6.0, ((0, 4), (1, 24))),
        "kv_latent": gaussian(arg_keys[1], (LAYERS, TOKENS, D_KV + ROPE), 1.0, 6.0, ((0, 4), (1, 24))),
        "segment_ids": jnp.searchsorted(jnp.cumsum(ragged_sizes(arg_keys[2], max(4, TOKENS // 64), TOKENS, min(512, TOKENS // 2), 1)), jnp.arange(TOKENS), side="right").astype(jnp.int32),
        "q_weight": draw_q_weight(jax.random.fold_in(arg_keys[5], 71), 0),
        "k_weight": gaussian(arg_keys[4], (LAYERS, D_KV, HEADS * NOPE), D_KV ** -0.5, 0.25, ((0, 4), (2, 8))),
    }


clip_threshold = 100.0
rope_base = 50000.0

def rotate(values, positions):
    half_width = values.shape[-1] // 2
    frequency = rope_base ** (-jnp.arange(half_width, dtype=jnp.float32) / half_width)
    angles = positions[:, None].astype(jnp.float32) * frequency[None, :]
    cosine = jnp.cos(angles)[:, None, :]
    sine_part = jnp.sin(angles)[:, None, :]
    lower_half = values[..., :half_width]
    upper_half = values[..., half_width:]
    return jnp.concatenate([lower_half * cosine - upper_half * sine_part, upper_half * cosine + lower_half * sine_part], -1)

def sequence_maxima(q_full, kv_rows, segments, w_key):
    length = kv_rows.shape[0]
    heads_here = w_key.shape[1] // NOPE
    q_full = q_full.reshape(length, heads_here, NOPE + ROPE)
    positions = jnp.arange(length, dtype=jnp.int32)
    queries = jnp.concatenate([q_full[..., :NOPE], rotate(q_full[..., NOPE:], positions)], -1).astype(jnp.bfloat16)
    key_nope = jnp.dot(kv_rows[:, :D_KV], w_key, preferred_element_type=jnp.float32).astype(jnp.bfloat16)
    key_nope = key_nope.reshape(length, heads_here, NOPE)
    key_rope = jnp.broadcast_to(kv_rows[:, None, D_KV:], (length, heads_here, ROPE))
    keys_all = jnp.concatenate([key_nope, key_rope], -1)
    logits = jnp.einsum('shd,thd->hst', queries.astype(jnp.float32), keys_all.astype(jnp.float32))
    logits = logits * (NOPE + ROPE) ** (-0.5)
    allowed = (segments[:, None] == segments[None, :]) & (positions[None, :] <= positions[:, None])
    return lax.optimization_barrier(jnp.max(jnp.where(allowed[None], logits, -1e+30), axis=(1, 2)))

def scale_weights(own_max, q_weight, k_weight):
    factor = clip_threshold / jnp.maximum(own_max, clip_threshold)
    square_root = jnp.sqrt(factor)
    layers_here, heads_here = own_max.shape
    column_scale = jnp.concatenate([jnp.broadcast_to(square_root[..., None], (layers_here, heads_here, NOPE)), jnp.broadcast_to(factor[..., None], (layers_here, heads_here, ROPE))], -1)
    rows_q = q_weight.shape[1]
    scaled_q = (q_weight.astype(jnp.float32).reshape(layers_here, rows_q, heads_here, NOPE + ROPE) * column_scale[:, None]).reshape(q_weight.shape).astype(jnp.bfloat16)
    scaled_k = (k_weight.astype(jnp.float32).reshape(layers_here, D_KV, heads_here, NOPE) * square_root[:, None, :, None]).reshape(k_weight.shape).astype(jnp.bfloat16)
    return (scaled_q, scaled_k)

def reference(q_latent, kv_latent, segment_ids, q_weight, k_weight):
    seg_rows = segment_ids.reshape(N_DP, SEQ)
    layer_rows = []
    for layer_idx in range(LAYERS):
        w_query = q_weight[layer_idx]
        w_key = k_weight[layer_idx]

        def one_sequence(inputs):
            latent_q, kv_rows, segments = inputs
            q_full = jnp.dot(latent_q, w_query, preferred_element_type=jnp.float32)
            return sequence_maxima(q_full, kv_rows, segments, w_key)
        per_sequence = lax.map(one_sequence, (q_latent[layer_idx].reshape(N_DP, SEQ, D_Q), kv_latent[layer_idx].reshape(N_DP, SEQ, D_KV + ROPE), seg_rows))
        layer_rows.append(lax.optimization_barrier(jnp.max(per_sequence, axis=0)))
    max_table = jnp.stack(layer_rows)
    scaled_q, scaled_k = scale_weights(max_table, q_weight, k_weight)
    return (max_table / clip_threshold, scaled_q, scaled_k)
```

```python
import jax
import jax.numpy as jnp
import numpy as np
from jax import lax
from jax.experimental import pallas as pl
from jax.experimental.pallas import tpu as pltpu
from jax.sharding import PartitionSpec as P

D_Q = 1536
D_KV = 512
NOPE = 128
ROPE = 64
HEAD = NOPE + ROPE
SEQ = 512

clip_threshold = 100.0
rope_base = 50000.0
wire_scale = 512.0
masked = -1e30


def rope_tables():
    half = ROPE // 2
    frequency = np.float32(rope_base) ** (-np.arange(half, dtype=np.float32) / np.float32(half))
    angles = np.arange(SEQ, dtype=np.float32)[:, None] * frequency[None, :].astype(np.float32)
    cosine = np.cos(angles.astype(np.float64)).astype(np.float32)
    sine = np.sin(angles.astype(np.float64)).astype(np.float32)
    return np.tile(cosine, (1, 4)), np.concatenate([-sine, sine, -sine, sine], 1)


def maxima_kernel(a_ref, w_ref, kv_ref, kw_ref, seg_ref, cos_ref, sin_ref, o_ref, q_ref, kc_ref, bias_ref, top_ref):
    heads = kw_ref.shape[1] // NOPE
    lane = lax.broadcasted_iota(jnp.int32, (SEQ, 128), 1)
    low = lane < 64
    keys = lax.dot_general(
        kw_ref[...], kv_ref[0:D_KV, :], (((0,), (0,)), ((), ())), preferred_element_type=jnp.float32
    ).astype(jnp.bfloat16)
    shared = kv_ref[D_KV : D_KV + ROPE, :]
    nothing = jnp.zeros_like(shared)
    for h in range(heads):
        upper = keys[h * NOPE : h * NOPE + 64]
        lower = keys[h * NOPE + 64 : (h + 1) * NOPE]
        if h % 2 == 0:
            kc_ref[h] = jnp.concatenate([upper, lower, shared, nothing], 0)
        else:
            kc_ref[h] = jnp.concatenate([lower, upper, nothing, shared], 0)
    row = seg_ref[...].astype(jnp.float32)
    column = jnp.transpose(jnp.broadcast_to(row, (128, SEQ)))
    position = lax.broadcasted_iota(jnp.int32, (SEQ, 128), 0)
    for j in range(SEQ // 128):
        here = slice(j * 128, (j + 1) * 128)
        same = column == jnp.broadcast_to(row[:, here], (SEQ, 128))
        bias_ref[:, here] = jnp.where(same & (lane + j * 128 <= position), 0.0, masked)
    width = 4 * HEAD
    for g in range(heads // 4):
        q_ref[...] = jnp.dot(a_ref[...], w_ref[:, g * width : (g + 1) * width], preferred_element_type=jnp.float32)
        for p in range(2):
            first = q_ref[:, p * 384 : p * 384 + 128]
            second = q_ref[:, p * 384 + 128 : p * 384 + 256]
            third = q_ref[:, p * 384 + 256 : p * 384 + 384]
            turn = jnp.where(low, second, third)
            partner = jnp.where(lane % 64 < 32, pltpu.roll(turn, 96, 1), pltpu.roll(turn, 32, 1))
            turned = (turn * cos_ref[...] + partner * sin_ref[...]).astype(jnp.bfloat16)
            swapped = jnp.where(low, third, second)
            for i, part in enumerate((first, swapped)):
                h = 4 * g + 2 * p + i
                query = jnp.concatenate([part.astype(jnp.bfloat16), turned], 1)
                top = None
                for s0, s1, t1 in ((0, 256, 256), (256, 512, 512)):
                    x = jnp.dot(query[s0:s1], kc_ref[h, :, 0:t1], preferred_element_type=jnp.float32)
                    x = x + bias_ref[s0:s1, 0:t1]
                    for t in range(0, t1, 128):
                        y = jnp.max(x[:, t : t + 128].reshape(32, 8, 128), axis=0)
                        top = y if top is None else jnp.maximum(top, y)
                top_ref[h] = top
    spot = lax.broadcasted_iota(jnp.int32, (1, 128), 1)
    out = jnp.zeros((1, 128), jnp.float32)
    for h in range(heads):
        best = jnp.max(jnp.max(top_ref[h], axis=0, keepdims=True), axis=1, keepdims=True)
        out = jnp.where(spot == h, best, out)
    out = out * (1.0 / wire_scale) * HEAD ** (-0.5)
    o_ref[...] = jnp.broadcast_to(out[:, :heads].reshape(1, 1, heads), o_ref.shape)


def local_maxima(a, w, kv, kw, seg, copies):
    cosine, sine = rope_tables()
    heads = kw.shape[1] // NOPE
    vmem = pl.BlockSpec(memory_space=pltpu.VMEM)
    return pl.pallas_call(
        maxima_kernel,
        out_shape=jax.ShapeDtypeStruct((copies, 1, heads), jnp.float32),
        in_specs=[vmem] * 7,
        out_specs=vmem,
        scratch_shapes=[
            pltpu.VMEM((SEQ, 4 * HEAD), jnp.float32),
            pltpu.VMEM((heads, 256, SEQ), jnp.bfloat16),
            pltpu.VMEM((SEQ, SEQ), jnp.float32),
            pltpu.VMEM((heads, 8, 128), jnp.float32),
        ],
        compiler_params=pltpu.CompilerParams(vmem_limit_bytes=32 << 20),
    )(a, w, kv, kw, seg, jnp.asarray(cosine), jnp.asarray(sine))


def finish_kernel(section_ref, all_ref, wq_ref, wk_ref, ratio_ref, sq_ref, sk_ref):
    layers, heads = ratio_ref.shape
    own = jnp.zeros((1, heads), jnp.float32)
    for s in range(layers):
        best = all_ref[s]
        for d in range(1, all_ref.shape[0] // layers):
            best = jnp.maximum(best, all_ref[d * layers + s])
        ratio_ref[s : s + 1, :] = best / clip_threshold
        own = jnp.where(section_ref[0] == s, best, own)
    factor = clip_threshold / jnp.maximum(own, clip_threshold)
    root = jnp.sqrt(factor)
    column = lax.broadcasted_iota(jnp.int32, (1, wq_ref.shape[1]), 1)
    scale = jnp.zeros((1, wq_ref.shape[1]), jnp.float32)
    for h in range(heads):
        scale = jnp.where(column >= h * HEAD, root[:, h : h + 1], scale)
        scale = jnp.where(column >= h * HEAD + NOPE, factor[:, h : h + 1], scale)
    sq_ref[...] = (wq_ref[...].astype(jnp.float32) * scale).astype(jnp.bfloat16)
    for h in range(heads):
        here = slice(h * NOPE, (h + 1) * NOPE)
        sk_ref[:, here] = (wk_ref[:, here].astype(jnp.float32) * root[:, h : h + 1]).astype(jnp.bfloat16)


def finish(section, everything, wq, wk, layers):
    vmem = pl.BlockSpec(memory_space=pltpu.VMEM)
    return pl.pallas_call(
        finish_kernel,
        out_shape=(
            jax.ShapeDtypeStruct((layers, everything.shape[2]), jnp.float32),
            jax.ShapeDtypeStruct(wq.shape, jnp.bfloat16),
            jax.ShapeDtypeStruct(wk.shape, jnp.bfloat16),
        ),
        in_specs=[pl.BlockSpec(memory_space=pltpu.SMEM), vmem, vmem, vmem],
        out_specs=(vmem, vmem, vmem),
    )(section, everything, wq, wk)


def per_device(q_latent, kv_latent, segment_ids, q_weight, k_weight):
    layers = lax.axis_size("section")
    copies = lax.axis_size("dp") * layers
    sent = (q_weight[0].astype(jnp.float32) * wire_scale).astype(jnp.float16)
    gathered = lax.all_gather(sent, "dp", axis=0, tiled=True).astype(jnp.bfloat16)
    kv = jnp.swapaxes(kv_latent[0], 0, 1)
    own = local_maxima(q_latent[0], gathered, kv, k_weight[0], segment_ids.reshape(1, -1), copies)
    everything = lax.all_to_all(own, ("dp", "section"), 0, 0, tiled=True)
    section = lax.axis_index("section").astype(jnp.int32).reshape(1)
    ratio, scaled_q, scaled_k = finish(section, everything, q_weight[0], k_weight[0], layers)
    return ratio, scaled_q[None], scaled_k[None]


def solution(mesh):
    return jax.shard_map(
        per_device,
        mesh=mesh,
        in_specs=(
            P("section", "dp", None),
            P("section", "dp", None),
            P("dp"),
            P("section", "dp", "head"),
            P("section", None, "head"),
        ),
        out_specs=(P(None, "head"), P("section", "dp", "head"), P("section", None, "head")),
        check_vma=False,
    )
```

```python
import jax
import jax.numpy as jnp
import numpy as np
from jax import lax
from jax.experimental import pallas as pl
from jax.experimental.pallas import tpu as pltpu
from jax.sharding import PartitionSpec as P

D_Q = 1536
D_KV = 512
NOPE = 128
ROPE = 64
HEAD = NOPE + ROPE
SEQ = 512

clip_threshold = 100.0
rope_base = 50000.0
wire_scale = 512.0
masked = -1e30


def rope_tables():
    half = ROPE // 2
    frequency = np.float32(rope_base) ** (-np.arange(half, dtype=np.float32) / np.float32(half))
    angles = np.arange(SEQ, dtype=np.float32)[:, None] * frequency[None, :].astype(np.float32)
    cosine = np.cos(angles.astype(np.float64)).astype(np.float32)
    sine = np.sin(angles.astype(np.float64)).astype(np.float32)
    return np.tile(cosine, (1, 4)), np.concatenate([-sine, sine, -sine, sine], 1)


def maxima_kernel(a_ref, w_ref, kv_ref, kw_ref, seg_ref, cos_ref, sin_ref, o_ref, q_ref, kc_ref, bias_ref, top_ref):
    heads = kw_ref.shape[1] // NOPE
    lane = lax.broadcasted_iota(jnp.int32, (SEQ, 128), 1)
    low = lane < 64
    keys = lax.dot_general(
        kw_ref[...], kv_ref[0:D_KV, :], (((0,), (0,)), ((), ())), preferred_element_type=jnp.float32
    ).astype(jnp.bfloat16)
    shared = kv_ref[D_KV : D_KV + ROPE, :]
    nothing = jnp.zeros_like(shared)
    for h in range(heads):
        upper = keys[h * NOPE : h * NOPE + 64]
        lower = keys[h * NOPE + 64 : (h + 1) * NOPE]
        if h % 2 == 0:
            kc_ref[h] = jnp.concatenate([upper, lower, shared, nothing], 0)
        else:
            kc_ref[h] = jnp.concatenate([lower, upper, nothing, shared], 0)
    row = seg_ref[...].astype(jnp.float32)
    column = jnp.transpose(jnp.broadcast_to(row, (128, SEQ)))
    position = lax.broadcasted_iota(jnp.int32, (SEQ, 128), 0)
    for j in range(SEQ // 128):
        here = slice(j * 128, (j + 1) * 128)
        same = column == jnp.broadcast_to(row[:, here], (SEQ, 128))
        bias_ref[:, here] = jnp.where(same & (lane + j * 128 <= position), 0.0, masked)
    width = 4 * HEAD
    for g in range(heads // 4):
        q_ref[...] = jnp.dot(a_ref[...], w_ref[:, g * width : (g + 1) * width], preferred_element_type=jnp.float32)
        for p in range(2):
            first = q_ref[:, p * 384 : p * 384 + 128]
            second = q_ref[:, p * 384 + 128 : p * 384 + 256]
            third = q_ref[:, p * 384 + 256 : p * 384 + 384]
            turn = jnp.where(low, second, third)
            partner = jnp.where(lane % 64 < 32, pltpu.roll(turn, 96, 1), pltpu.roll(turn, 32, 1))
            turned = (turn * cos_ref[...] + partner * sin_ref[...]).astype(jnp.bfloat16)
            swapped = jnp.where(low, third, second)
            for i, part in enumerate((first, swapped)):
                h = 4 * g + 2 * p + i
                query = jnp.concatenate([part.astype(jnp.bfloat16), turned], 1)
                top = None
                for s0, s1, t1 in ((0, 256, 256), (256, 512, 512)):
                    x = jnp.dot(query[s0:s1], kc_ref[h, :, 0:t1], preferred_element_type=jnp.float32)
                    x = x + bias_ref[s0:s1, 0:t1]
                    for t in range(0, t1, 128):
                        y = jnp.max(x[:, t : t + 128].reshape(32, 8, 128), axis=0)
                        top = y if top is None else jnp.maximum(top, y)
                top_ref[h] = top
    spot = lax.broadcasted_iota(jnp.int32, (1, 128), 1)
    out = jnp.zeros((1, 128), jnp.float32)
    for h in range(heads):
        best = jnp.max(jnp.max(top_ref[h], axis=0, keepdims=True), axis=1, keepdims=True)
        out = jnp.where(spot == h, best, out)
    out = out * (1.0 / wire_scale) * HEAD ** (-0.5)
    o_ref[...] = jnp.broadcast_to(out[:, :heads].reshape(1, 1, heads), o_ref.shape)


def local_maxima(a, w, kv, kw, seg, copies):
    cosine, sine = rope_tables()
    heads = kw.shape[1] // NOPE
    vmem = pl.BlockSpec(memory_space=pltpu.VMEM)
    return pl.pallas_call(
        maxima_kernel,
        out_shape=jax.ShapeDtypeStruct((copies, 1, heads), jnp.float32),
        in_specs=[vmem] * 7,
        out_specs=vmem,
        scratch_shapes=[
            pltpu.VMEM((SEQ, 4 * HEAD), jnp.float32),
            pltpu.VMEM((heads, 256, SEQ), jnp.bfloat16),
            pltpu.VMEM((SEQ, SEQ), jnp.float32),
            pltpu.VMEM((heads, 8, 128), jnp.float32),
        ],
        compiler_params=pltpu.CompilerParams(vmem_limit_bytes=32 << 20),
    )(a, w, kv, kw, seg, jnp.asarray(cosine), jnp.asarray(sine))


def finish_kernel(section_ref, all_ref, wq_ref, wk_ref, ratio_ref, sq_ref, sk_ref):
    layers, heads = ratio_ref.shape
    own = jnp.zeros((1, heads), jnp.float32)
    for s in range(layers):
        best = all_ref[s]
        for d in range(1, all_ref.shape[0] // layers):
            best = jnp.maximum(best, all_ref[d * layers + s])
        ratio_ref[s : s + 1, :] = best / clip_threshold
        own = jnp.where(section_ref[0] == s, best, own)
    factor = clip_threshold / jnp.maximum(own, clip_threshold)
    root = jnp.sqrt(factor)
    column = lax.broadcasted_iota(jnp.int32, (1, wq_ref.shape[1]), 1)
    scale = jnp.zeros((1, wq_ref.shape[1]), jnp.float32)
    for h in range(heads):
        scale = jnp.where(column >= h * HEAD, root[:, h : h + 1], scale)
        scale = jnp.where(column >= h * HEAD + NOPE, factor[:, h : h + 1], scale)
    sq_ref[...] = (wq_ref[...].astype(jnp.float32) * scale).astype(jnp.bfloat16)
    for h in range(heads):
        here = slice(h * NOPE, (h + 1) * NOPE)
        sk_ref[:, here] = (wk_ref[:, here].astype(jnp.float32) * root[:, h : h + 1]).astype(jnp.bfloat16)


def finish(section, everything, wq, wk, layers):
    vmem = pl.BlockSpec(memory_space=pltpu.VMEM)
    return pl.pallas_call(
        finish_kernel,
        out_shape=(
            jax.ShapeDtypeStruct((layers, everything.shape[2]), jnp.float32),
            jax.ShapeDtypeStruct(wq.shape, jnp.bfloat16),
            jax.ShapeDtypeStruct(wk.shape, jnp.bfloat16),
        ),
        in_specs=[pl.BlockSpec(memory_space=pltpu.SMEM), vmem, vmem, vmem],
        out_specs=(vmem, vmem, vmem),
        compiler_params=pltpu.CompilerParams(vmem_limit_bytes=8 << 20),
    )(section, everything, wq, wk)


def per_device(q_latent, kv_latent, segment_ids, q_weight, k_weight):
    layers = lax.axis_size("section")
    copies = lax.axis_size("dp") * layers
    sent = (q_weight[0].astype(jnp.float32) * wire_scale).astype(jnp.float16)
    section = lax.axis_index("section").astype(jnp.int32).reshape(1)
    section, sent = lax.optimization_barrier((section, sent))
    gathered = lax.all_gather(sent, "dp", axis=0, tiled=True).astype(jnp.bfloat16)
    kv = jnp.swapaxes(kv_latent[0], 0, 1)
    own = local_maxima(q_latent[0], gathered, kv, k_weight[0], segment_ids.reshape(1, -1), copies)
    everything = lax.all_to_all(own, ("dp", "section"), 0, 0, tiled=True)
    ratio, scaled_q, scaled_k = finish(section, everything, q_weight[0], k_weight[0], layers)
    return ratio, scaled_q[None], scaled_k[None]


def solution(mesh):
    return jax.shard_map(
        per_device,
        mesh=mesh,
        in_specs=(
            P("section", "dp", None),
            P("section", "dp", None),
            P("dp"),
            P("section", "dp", "head"),
            P("section", None, "head"),
        ),
        out_specs=(P(None, "head"), P("section", "dp", "head"), P("section", None, "head")),
        check_vma=False,
    )
```

```python
import jax
import jax.numpy as jnp
import numpy as np
from jax import lax
from jax.experimental import pallas as pl
from jax.experimental.pallas import tpu as pltpu
from jax.sharding import PartitionSpec as P

D_Q = 1536
D_KV = 512
NOPE = 128
ROPE = 64
HEAD = NOPE + ROPE
SEQ = 512

clip_threshold = 100.0
rope_base = 50000.0
wire_scale = 512.0
masked = -1e30


def rope_tables():
    half = ROPE // 2
    frequency = np.float32(rope_base) ** (-np.arange(half, dtype=np.float32) / np.float32(half))
    angles = np.arange(SEQ, dtype=np.float32)[:, None] * frequency[None, :].astype(np.float32)
    cosine = np.cos(angles.astype(np.float64)).astype(np.float32)
    sine = np.sin(angles.astype(np.float64)).astype(np.float32)
    return np.tile(cosine, (1, 4)), np.concatenate([-sine, sine, -sine, sine], 1)


def maxima_kernel(q_ref, kv_ref, kw_ref, seg_ref, cos_ref, sin_ref, o_ref, kc_ref, bias_ref, top_ref):
    heads = kw_ref.shape[1] // NOPE
    lane = lax.broadcasted_iota(jnp.int32, (SEQ, 128), 1)
    low = lane < 64
    keys = lax.dot_general(
        kw_ref[...], kv_ref[0:D_KV, :], (((0,), (0,)), ((), ())), preferred_element_type=jnp.float32
    ).astype(jnp.bfloat16)
    shared = kv_ref[D_KV : D_KV + ROPE, :]
    nothing = jnp.zeros_like(shared)
    for h in range(heads):
        upper = keys[h * NOPE : h * NOPE + 64]
        lower = keys[h * NOPE + 64 : (h + 1) * NOPE]
        if h % 2 == 0:
            kc_ref[h] = jnp.concatenate([upper, lower, shared, nothing], 0)
        else:
            kc_ref[h] = jnp.concatenate([lower, upper, nothing, shared], 0)
    row = seg_ref[...].astype(jnp.float32)
    column = jnp.transpose(jnp.broadcast_to(row, (128, SEQ)))
    position = lax.broadcasted_iota(jnp.int32, (SEQ, 128), 0)
    for j in range(SEQ // 128):
        here = slice(j * 128, (j + 1) * 128)
        same = column == jnp.broadcast_to(row[:, here], (SEQ, 128))
        bias_ref[:, here] = jnp.where(same & (lane + j * 128 <= position), 0.0, masked)
    for g in range(heads // 4):
        for p in range(2 * g, 2 * g + 2):
            first = q_ref[:, p * 384 : p * 384 + 128]
            second = q_ref[:, p * 384 + 128 : p * 384 + 256]
            third = q_ref[:, p * 384 + 256 : p * 384 + 384]
            turn = jnp.where(low, second, third)
            partner = jnp.where(lane % 64 < 32, pltpu.roll(turn, 96, 1), pltpu.roll(turn, 32, 1))
            turned = (turn * cos_ref[...] + partner * sin_ref[...]).astype(jnp.bfloat16)
            swapped = jnp.where(low, third, second)
            for i, part in enumerate((first, swapped)):
                h = 2 * p + i
                query = jnp.concatenate([part.astype(jnp.bfloat16), turned], 1)
                top = None
                for s0, s1, t1 in ((0, 256, 256), (256, 512, 512)):
                    x = jnp.dot(query[s0:s1], kc_ref[h, :, 0:t1], preferred_element_type=jnp.float32)
                    x = x + bias_ref[s0:s1, 0:t1]
                    for t in range(0, t1, 128):
                        y = jnp.max(x[:, t : t + 128].reshape(32, 8, 128), axis=0)
                        top = y if top is None else jnp.maximum(top, y)
                top_ref[h] = top
    spot = lax.broadcasted_iota(jnp.int32, (1, 128), 1)
    out = jnp.zeros((1, 128), jnp.float32)
    for h in range(heads):
        best = jnp.max(jnp.max(top_ref[h], axis=0, keepdims=True), axis=1, keepdims=True)
        out = jnp.where(spot == h, best, out)
    out = out * (1.0 / wire_scale) * HEAD ** (-0.5)
    o_ref[...] = jnp.broadcast_to(out[:, :heads].reshape(1, 1, heads), o_ref.shape)


def local_maxima(q, kv, kw, seg, copies):
    cosine, sine = rope_tables()
    heads = kw.shape[1] // NOPE
    vmem = pl.BlockSpec(memory_space=pltpu.VMEM)
    return pl.pallas_call(
        maxima_kernel,
        out_shape=jax.ShapeDtypeStruct((copies, 1, heads), jnp.float32),
        in_specs=[vmem] * 6,
        out_specs=vmem,
        scratch_shapes=[
            pltpu.VMEM((heads, 256, SEQ), jnp.bfloat16),
            pltpu.VMEM((SEQ, SEQ), jnp.float32),
            pltpu.VMEM((heads, 8, 128), jnp.float32),
        ],
        compiler_params=pltpu.CompilerParams(vmem_limit_bytes=16 << 20),
    )(q, kv, kw, seg, jnp.asarray(cosine), jnp.asarray(sine))


def finish_kernel(section_ref, all_ref, wq_ref, wk_ref, ratio_ref, sq_ref, sk_ref):
    layers, heads = ratio_ref.shape
    own = jnp.zeros((1, heads), jnp.float32)
    for s in range(layers):
        best = all_ref[s]
        for d in range(1, all_ref.shape[0] // layers):
            best = jnp.maximum(best, all_ref[d * layers + s])
        ratio_ref[s : s + 1, :] = best / clip_threshold
        own = jnp.where(section_ref[0] == s, best, own)
    factor = clip_threshold / jnp.maximum(own, clip_threshold)
    root = jnp.sqrt(factor)
    column = lax.broadcasted_iota(jnp.int32, (1, wq_ref.shape[1]), 1)
    scale = jnp.zeros((1, wq_ref.shape[1]), jnp.float32)
    for h in range(heads):
        scale = jnp.where(column >= h * HEAD, root[:, h : h + 1], scale)
        scale = jnp.where(column >= h * HEAD + NOPE, factor[:, h : h + 1], scale)
    sq_ref[...] = (wq_ref[...].astype(jnp.float32) * scale).astype(jnp.bfloat16)
    for h in range(heads):
        here = slice(h * NOPE, (h + 1) * NOPE)
        sk_ref[:, here] = (wk_ref[:, here].astype(jnp.float32) * root[:, h : h + 1]).astype(jnp.bfloat16)


def finish(section, everything, wq, wk, layers):
    vmem = pl.BlockSpec(memory_space=pltpu.VMEM)
    return pl.pallas_call(
        finish_kernel,
        out_shape=(
            jax.ShapeDtypeStruct((layers, everything.shape[2]), jnp.float32),
            jax.ShapeDtypeStruct(wq.shape, jnp.bfloat16),
            jax.ShapeDtypeStruct(wk.shape, jnp.bfloat16),
        ),
        in_specs=[pl.BlockSpec(memory_space=pltpu.SMEM), vmem, vmem, vmem],
        out_specs=(vmem, vmem, vmem),
        compiler_params=pltpu.CompilerParams(vmem_limit_bytes=8 << 20),
    )(section, everything, wq, wk)


def per_device(q_latent, kv_latent, segment_ids, q_weight, k_weight):
    layers = lax.axis_size("section")
    copies = lax.axis_size("dp") * layers
    sent = (q_weight[0].astype(jnp.float32) * wire_scale).astype(jnp.float16)
    section = lax.axis_index("section").astype(jnp.int32).reshape(1)
    section, sent = lax.optimization_barrier((section, sent))
    gathered = lax.all_gather(sent, "dp", axis=0, tiled=True).astype(jnp.bfloat16)
    kv = jnp.swapaxes(kv_latent[0], 0, 1)
    q = jnp.dot(q_latent[0], gathered, preferred_element_type=jnp.float32)
    own = local_maxima(q, kv, k_weight[0], segment_ids.reshape(1, -1), copies)
    everything = lax.all_to_all(own, ("dp", "section"), 0, 0, tiled=True)
    ratio, scaled_q, scaled_k = finish(section, everything, q_weight[0], k_weight[0], layers)
    return ratio, scaled_q[None], scaled_k[None]


def solution(mesh):
    return jax.shard_map(
        per_device,
        mesh=mesh,
        in_specs=(
            P("section", "dp", None),
            P("section", "dp", None),
            P("dp"),
            P("section", "dp", "head"),
            P("section", None, "head"),
        ),
        out_specs=(P(None, "head"), P("section", "dp", "head"), P("section", None, "head")),
        check_vma=False,
    )
```

```python
import jax
import jax.numpy as jnp
import numpy as np
from jax import lax
from jax.experimental import pallas as pl
from jax.experimental.pallas import tpu as pltpu
from jax.sharding import PartitionSpec as P

D_Q = 1536
D_KV = 512
NOPE = 128
ROPE = 64
HEAD = NOPE + ROPE
SEQ = 512

clip_threshold = 100.0
rope_base = 50000.0
wire_scale = 512.0
masked = -1e30


def rope_tables():
    half = ROPE // 2
    frequency = np.float32(rope_base) ** (-np.arange(half, dtype=np.float32) / np.float32(half))
    angles = np.arange(SEQ, dtype=np.float32)[:, None] * frequency[None, :].astype(np.float32)
    cosine = np.cos(angles.astype(np.float64)).astype(np.float32)
    sine = np.sin(angles.astype(np.float64)).astype(np.float32)
    return np.tile(cosine, (1, 4)), np.concatenate([-sine, sine, -sine, sine], 1)


def maxima_kernel(q_ref, kv_ref, kw_ref, seg_ref, cos_ref, sin_ref, o_ref, kc_ref, bias_ref, top_ref):
    heads = kw_ref.shape[1] // NOPE
    lane = lax.broadcasted_iota(jnp.int32, (SEQ, 128), 1)
    low = lane < 64
    keys = lax.dot_general(
        kw_ref[...], kv_ref[0:D_KV, :], (((0,), (0,)), ((), ())), preferred_element_type=jnp.float32
    ).astype(jnp.bfloat16)
    shared = kv_ref[D_KV : D_KV + ROPE, :]
    nothing = jnp.zeros_like(shared)
    for h in range(heads):
        upper = keys[h * NOPE : h * NOPE + 64]
        lower = keys[h * NOPE + 64 : (h + 1) * NOPE]
        if h % 2 == 0:
            kc_ref[h] = jnp.concatenate([upper, lower, shared, nothing], 0)
        else:
            kc_ref[h] = jnp.concatenate([lower, upper, nothing, shared], 0)
    row = seg_ref[...].astype(jnp.float32)
    column = jnp.transpose(jnp.broadcast_to(row, (128, SEQ)))
    position = lax.broadcasted_iota(jnp.int32, (SEQ, 128), 0)
    for j in range(SEQ // 128):
        here = slice(j * 128, (j + 1) * 128)
        same = column == jnp.broadcast_to(row[:, here], (SEQ, 128))
        bias_ref[:, here] = jnp.where(same & (lane + j * 128 <= position), 0.0, masked)
    for g in range(heads // 4):
        for p in range(2 * g, 2 * g + 2):
            first = q_ref[:, p * 384 : p * 384 + 128]
            second = q_ref[:, p * 384 + 128 : p * 384 + 256]
            third = q_ref[:, p * 384 + 256 : p * 384 + 384]
            turn = jnp.where(low, second, third)
            partner = jnp.where(lane % 64 < 32, pltpu.roll(turn, 96, 1), pltpu.roll(turn, 32, 1))
            turned = (turn * cos_ref[...] + partner * sin_ref[...]).astype(jnp.bfloat16)
            swapped = jnp.where(low, third, second)
            for i, part in enumerate((first, swapped)):
                h = 2 * p + i
                query = jnp.concatenate([part.astype(jnp.bfloat16), turned], 1)
                top = None
                for s0, s1, t1 in ((0, 256, 256), (256, 512, 512)):
                    x = jnp.dot(query[s0:s1], kc_ref[h, :, 0:t1], preferred_element_type=jnp.float32)
                    x = x + bias_ref[s0:s1, 0:t1]
                    for t in range(0, t1, 128):
                        y = jnp.max(x[:, t : t + 128].reshape(32, 8, 128), axis=0)
                        top = y if top is None else jnp.maximum(top, y)
                top_ref[h] = top
    spot = lax.broadcasted_iota(jnp.int32, (1, 128), 1)
    out = jnp.zeros((1, 128), jnp.float32)
    for h in range(heads):
        best = jnp.max(jnp.max(top_ref[h], axis=0, keepdims=True), axis=1, keepdims=True)
        out = jnp.where(spot == h, best, out)
    out = out * (1.0 / wire_scale) * HEAD ** (-0.5)
    o_ref[...] = jnp.broadcast_to(out[:, :heads].reshape(1, 1, heads), o_ref.shape)


def local_maxima(q, kv, kw, seg, copies):
    cosine, sine = rope_tables()
    heads = kw.shape[1] // NOPE
    vmem = pl.BlockSpec(memory_space=pltpu.VMEM)
    return pl.pallas_call(
        maxima_kernel,
        out_shape=jax.ShapeDtypeStruct((copies, 1, heads), jnp.float32),
        in_specs=[vmem] * 6,
        out_specs=vmem,
        scratch_shapes=[
            pltpu.VMEM((heads, 256, SEQ), jnp.bfloat16),
            pltpu.VMEM((SEQ, SEQ), jnp.float32),
            pltpu.VMEM((heads, 8, 128), jnp.float32),
        ],
        compiler_params=pltpu.CompilerParams(vmem_limit_bytes=16 << 20),
    )(q, kv, kw, seg, jnp.asarray(cosine), jnp.asarray(sine))


def finish_kernel(all_ref, wq_ref, wk_ref, ratio_ref, sq_ref, sk_ref):
    layers, heads = ratio_ref.shape
    section = lax.axis_index("section")
    own = jnp.zeros((1, heads), jnp.float32)
    for s in range(layers):
        best = all_ref[s]
        for d in range(1, all_ref.shape[0] // layers):
            best = jnp.maximum(best, all_ref[d * layers + s])
        ratio_ref[s : s + 1, :] = best / clip_threshold
        own = jnp.where(section == s, best, own)
    factor = clip_threshold / jnp.maximum(own, clip_threshold)
    root = jnp.sqrt(factor)
    column = lax.broadcasted_iota(jnp.int32, (1, wq_ref.shape[1]), 1)
    scale = jnp.zeros((1, wq_ref.shape[1]), jnp.float32)
    for h in range(heads):
        scale = jnp.where(column >= h * HEAD, root[:, h : h + 1], scale)
        scale = jnp.where(column >= h * HEAD + NOPE, factor[:, h : h + 1], scale)
    sq_ref[...] = (wq_ref[...].astype(jnp.float32) * scale).astype(jnp.bfloat16)
    for h in range(heads):
        here = slice(h * NOPE, (h + 1) * NOPE)
        sk_ref[:, here] = (wk_ref[:, here].astype(jnp.float32) * root[:, h : h + 1]).astype(jnp.bfloat16)


def finish(everything, wq, wk, layers):
    vmem = pl.BlockSpec(memory_space=pltpu.VMEM)
    return pl.pallas_call(
        finish_kernel,
        out_shape=(
            jax.ShapeDtypeStruct((layers, everything.shape[2]), jnp.float32),
            jax.ShapeDtypeStruct(wq.shape, jnp.bfloat16),
            jax.ShapeDtypeStruct(wk.shape, jnp.bfloat16),
        ),
        in_specs=[vmem, vmem, vmem],
        out_specs=(vmem, vmem, vmem),
        compiler_params=pltpu.CompilerParams(vmem_limit_bytes=8 << 20),
    )(everything, wq, wk)


def per_device(q_latent, kv_latent, segment_ids, q_weight, k_weight):
    layers = lax.axis_size("section")
    copies = lax.axis_size("dp") * layers
    sent = (q_weight[0].astype(jnp.float32) * wire_scale).astype(jnp.float16)
    gathered = lax.all_gather(sent, "dp", axis=0, tiled=True).astype(jnp.bfloat16)
    kv = jnp.swapaxes(kv_latent[0], 0, 1)
    q = jnp.dot(q_latent[0], gathered, preferred_element_type=jnp.float32)
    own = local_maxima(q, kv, k_weight[0], segment_ids.reshape(1, -1), copies)
    everything = lax.all_to_all(own, ("dp", "section"), 0, 0, tiled=True)
    ratio, scaled_q, scaled_k = finish(everything, q_weight[0], k_weight[0], layers)
    return ratio, scaled_q[None], scaled_k[None]


def solution(mesh):
    return jax.shard_map(
        per_device,
        mesh=mesh,
        in_specs=(
            P("section", "dp", None),
            P("section", "dp", None),
            P("dp"),
            P("section", "dp", "head"),
            P("section", None, "head"),
        ),
        out_specs=(P(None, "head"), P("section", "dp", "head"), P("section", None, "head")),
        check_vma=False,
    )
```

```python
import jax
import jax.numpy as jnp
import numpy as np
from jax import lax
from jax.experimental import pallas as pl
from jax.experimental.pallas import tpu as pltpu
from jax.sharding import PartitionSpec as P

D_Q = 1536
D_KV = 512
NOPE = 128
ROPE = 64
HEAD = NOPE + ROPE
SEQ = 512

clip_threshold = 100.0
rope_base = 50000.0
wire_scale = 512.0
masked = -1e30
PART = 128


def rope_tables():
    half = ROPE // 2
    frequency = np.float32(rope_base) ** (-np.arange(half, dtype=np.float32) / np.float32(half))
    angles = np.arange(SEQ, dtype=np.float32)[:, None] * frequency[None, :].astype(np.float32)
    cosine = np.cos(angles.astype(np.float64)).astype(np.float32)
    sine = np.sin(angles.astype(np.float64)).astype(np.float32)
    return np.tile(cosine, (1, 4)), np.concatenate([-sine, sine, -sine, sine], 1)


def maxima_kernel(q_ref, kv_ref, kw_ref, seg_ref, cos_ref, sin_ref, o_ref, kc_ref, bias_ref, top_ref):
    heads = kw_ref.shape[1] // NOPE
    lane = lax.broadcasted_iota(jnp.int32, (SEQ, 128), 1)
    low = lane < 64
    keys = lax.dot_general(
        kw_ref[...], kv_ref[0:D_KV, :], (((0,), (0,)), ((), ())), preferred_element_type=jnp.float32
    ).astype(jnp.bfloat16)
    shared = kv_ref[D_KV : D_KV + ROPE, :]
    nothing = jnp.zeros_like(shared)
    for h in range(heads):
        upper = keys[h * NOPE : h * NOPE + 64]
        lower = keys[h * NOPE + 64 : (h + 1) * NOPE]
        if h % 2 == 0:
            kc_ref[h] = jnp.concatenate([upper, lower, shared, nothing], 0)
        else:
            kc_ref[h] = jnp.concatenate([lower, upper, nothing, shared], 0)
    row = seg_ref[...].astype(jnp.float32)
    column = jnp.transpose(jnp.broadcast_to(row, (128, SEQ)))
    position = lax.broadcasted_iota(jnp.int32, (SEQ, 128), 0)
    for j in range(SEQ // 128):
        here = slice(j * 128, (j + 1) * 128)
        same = column == jnp.broadcast_to(row[:, here], (SEQ, 128))
        bias_ref[:, here] = jnp.where(same & (lane + j * 128 <= position), 0.0, masked)
    for g in range(heads // 4):
        for p in range(2 * g, 2 * g + 2):
            first = q_ref[:, p * 384 : p * 384 + 128]
            second = q_ref[:, p * 384 + 128 : p * 384 + 256]
            third = q_ref[:, p * 384 + 256 : p * 384 + 384]
            turn = jnp.where(low, second, third)
            partner = jnp.where(lane % 64 < 32, pltpu.roll(turn, 96, 1), pltpu.roll(turn, 32, 1))
            turned = (turn * cos_ref[...] + partner * sin_ref[...]).astype(jnp.bfloat16)
            swapped = jnp.where(low, third, second)
            for i, part in enumerate((first, swapped)):
                h = 2 * p + i
                query = jnp.concatenate([part.astype(jnp.bfloat16), turned], 1)
                top = None
                for s0, s1, t1 in ((0, 256, 256), (256, 512, 512)):
                    x = jnp.dot(query[s0:s1], kc_ref[h, :, 0:t1], preferred_element_type=jnp.float32)
                    x = x + bias_ref[s0:s1, 0:t1]
                    for t in range(0, t1, 128):
                        y = jnp.max(x[:, t : t + 128].reshape(32, 8, 128), axis=0)
                        top = y if top is None else jnp.maximum(top, y)
                top_ref[h] = top
    spot = lax.broadcasted_iota(jnp.int32, (1, 128), 1)
    out = jnp.zeros((1, 128), jnp.float32)
    for h in range(heads):
        best = jnp.max(jnp.max(top_ref[h], axis=0, keepdims=True), axis=1, keepdims=True)
        out = jnp.where(spot == h, best, out)
    out = out * (1.0 / wire_scale) * HEAD ** (-0.5)
    o_ref[...] = jnp.broadcast_to(out, o_ref.shape)


def local_maxima(q, kv, kw, seg, copies):
    cosine, sine = rope_tables()
    heads = kw.shape[1] // NOPE
    vmem = pl.BlockSpec(memory_space=pltpu.VMEM)
    return pl.pallas_call(
        maxima_kernel,
        out_shape=jax.ShapeDtypeStruct((copies, 128), jnp.float32),
        in_specs=[vmem] * 6,
        out_specs=vmem,
        scratch_shapes=[
            pltpu.VMEM((heads, 256, SEQ), jnp.bfloat16),
            pltpu.VMEM((SEQ, SEQ), jnp.float32),
            pltpu.VMEM((heads, 8, 128), jnp.float32),
        ],
        compiler_params=pltpu.CompilerParams(vmem_limit_bytes=16 << 20),
    )(q, kv, kw, seg, jnp.asarray(cosine), jnp.asarray(sine))


def finish_kernel(all_ref, wq_ref, wk_ref, ratio_hbm, sq_hbm, sk_hbm, ratio_ref, sq_ref, sk_ref, sems):
    layers, heads = ratio_ref.shape
    best = all_ref[0:8]
    for i in range(8, all_ref.shape[0], 8):
        best = jnp.maximum(best, all_ref[i : i + 8])
    best = jnp.maximum(best, pltpu.roll(best, 4, 0))
    ratio_ref[...] = best[0:layers, 0:heads] / clip_threshold
    row = lax.broadcasted_iota(jnp.int32, best.shape, 0)
    mine = jnp.where(row % layers == lax.axis_index("section"), best, -jnp.inf)
    own = jnp.max(mine, axis=0, keepdims=True)
    factor = clip_threshold / jnp.maximum(own, clip_threshold)
    root = jnp.sqrt(factor)
    column = lax.broadcasted_iota(jnp.int32, (1, wq_ref.shape[1]), 1)
    q_scale = jnp.zeros((1, wq_ref.shape[1]), jnp.float32)
    for h in range(heads):
        q_scale = jnp.where(column >= h * HEAD, root[:, h : h + 1], q_scale)
        q_scale = jnp.where(column >= h * HEAD + NOPE, factor[:, h : h + 1], q_scale)
    k_scale = jnp.concatenate([jnp.broadcast_to(root[:, h : h + 1], (1, NOPE)) for h in range(heads)], 1)

    def write(part):
        rows = pl.ds(pl.multiple_of(part * PART, PART), PART)
        return pltpu.make_async_copy(sk_ref.at[rows], sk_hbm.at[rows], sems.at[part])

    def scale(part, carry):
        rows = pl.ds(pl.multiple_of(part * PART, PART), PART)
        sk_ref[rows] = (wk_ref[rows].astype(jnp.float32) * k_scale).astype(jnp.bfloat16)

        @pl.when(part > 0)
        def _():
            write(part - 1).start()

        return carry

    parts = wk_ref.shape[0] // PART
    lax.fori_loop(0, parts, scale, 0)
    sq_ref[...] = (wq_ref[...].astype(jnp.float32) * q_scale).astype(jnp.bfloat16)
    write(parts - 1).start()
    others = [
        pltpu.make_async_copy(ratio_ref, ratio_hbm, sems.at[parts]),
        pltpu.make_async_copy(sq_ref, sq_hbm, sems.at[parts + 1]),
    ]
    for other in others:
        other.start()
    for part in range(parts):
        write(part).wait()
    for other in others:
        other.wait()


def finish(everything, wq, wk, layers):
    heads = wk.shape[1] // NOPE
    vmem = pl.BlockSpec(memory_space=pltpu.VMEM)
    away = pl.BlockSpec(memory_space=pl.ANY)
    return pl.pallas_call(
        finish_kernel,
        out_shape=(
            jax.ShapeDtypeStruct((layers, heads), jnp.float32),
            jax.ShapeDtypeStruct(wq.shape, jnp.bfloat16),
            jax.ShapeDtypeStruct(wk.shape, jnp.bfloat16),
        ),
        in_specs=[vmem, vmem, vmem],
        out_specs=(away, away, away),
        scratch_shapes=[
            pltpu.VMEM((layers, heads), jnp.float32),
            pltpu.VMEM(wq.shape, jnp.bfloat16),
            pltpu.VMEM(wk.shape, jnp.bfloat16),
            pltpu.SemaphoreType.DMA((wk.shape[0] // PART + 2,)),
        ],
        compiler_params=pltpu.CompilerParams(vmem_limit_bytes=8 << 20),
    )(everything, wq, wk)


def per_device(q_latent, kv_latent, segment_ids, q_weight, k_weight):
    layers = lax.axis_size("section")
    copies = lax.axis_size("dp") * layers
    sent = (q_weight[0].astype(jnp.float32) * wire_scale).astype(jnp.float16)
    gathered = lax.all_gather(sent, "dp", axis=0, tiled=True).astype(jnp.bfloat16)
    kv = jnp.swapaxes(kv_latent[0], 0, 1)
    q = jnp.dot(q_latent[0], gathered, preferred_element_type=jnp.float32)
    own = local_maxima(q, kv, k_weight[0], segment_ids.reshape(1, -1), copies)
    everything = lax.all_to_all(own.reshape(copies, 1, 128), ("dp", "section"), 0, 0, tiled=True)
    ratio, scaled_q, scaled_k = finish(everything.reshape(copies, 128), q_weight[0], k_weight[0], layers)
    return ratio, scaled_q[None], scaled_k[None]


def solution(mesh):
    return jax.shard_map(
        per_device,
        mesh=mesh,
        in_specs=(
            P("section", "dp", None),
            P("section", "dp", None),
            P("dp"),
            P("section", "dp", "head"),
            P("section", None, "head"),
        ),
        out_specs=(P(None, "head"), P("section", "dp", "head"), P("section", None, "head")),
        check_vma=False,
    )
```

```python
import jax
import jax.numpy as jnp
import numpy as np
from jax import lax
from jax.experimental import pallas as pl
from jax.experimental.pallas import tpu as pltpu
from jax.sharding import PartitionSpec as P

D_Q = 1536
D_KV = 512
NOPE = 128
ROPE = 64
HEAD = NOPE + ROPE
SEQ = 512

clip_threshold = 100.0
rope_base = 50000.0
wire_scale = 512.0
masked = -1e30
PART = 128


def rope_tables():
    half = ROPE // 2
    frequency = np.float32(rope_base) ** (-np.arange(half, dtype=np.float32) / np.float32(half))
    angles = np.arange(SEQ, dtype=np.float32)[:, None] * frequency[None, :].astype(np.float32)
    cosine = np.cos(angles.astype(np.float64)).astype(np.float32)
    sine = np.sin(angles.astype(np.float64)).astype(np.float32)
    return np.tile(cosine, (1, 4)), np.concatenate([-sine, sine, -sine, sine], 1)


def maxima_kernel(q_ref, kv_ref, kw_ref, seg_ref, cos_ref, sin_ref, o_ref, kc_ref, bias_ref, top_ref):
    heads = kw_ref.shape[1] // NOPE
    lane = lax.broadcasted_iota(jnp.int32, (SEQ, 128), 1)
    low = lane < 64
    keys = lax.dot_general(
        kw_ref[...], kv_ref[0:D_KV, :], (((0,), (0,)), ((), ())), preferred_element_type=jnp.float32
    ).astype(jnp.bfloat16)
    shared = kv_ref[D_KV : D_KV + ROPE, :]
    nothing = jnp.zeros_like(shared)
    for h in range(heads):
        upper = keys[h * NOPE : h * NOPE + 64]
        lower = keys[h * NOPE + 64 : (h + 1) * NOPE]
        if h % 2 == 0:
            kc_ref[h] = jnp.concatenate([upper, lower, shared, nothing], 0)
        else:
            kc_ref[h] = jnp.concatenate([lower, upper, nothing, shared], 0)
    row = seg_ref[...].astype(jnp.float32)
    column = jnp.transpose(jnp.broadcast_to(row, (128, SEQ)))
    position = lax.broadcasted_iota(jnp.int32, (SEQ, 128), 0)
    for j in range(SEQ // 128):
        here = slice(j * 128, (j + 1) * 128)
        same = column == jnp.broadcast_to(row[:, here], (SEQ, 128))
        bias_ref[:, here] = jnp.where(same & (lane + j * 128 <= position), 0.0, masked)
    for g in range(heads // 4):
        for p in range(2 * g, 2 * g + 2):
            first = q_ref[:, p * 384 : p * 384 + 128]
            second = q_ref[:, p * 384 + 128 : p * 384 + 256]
            third = q_ref[:, p * 384 + 256 : p * 384 + 384]
            turn = jnp.where(low, second, third)
            partner = jnp.where(lane % 64 < 32, pltpu.roll(turn, 96, 1), pltpu.roll(turn, 32, 1))
            turned = (turn * cos_ref[...] + partner * sin_ref[...]).astype(jnp.bfloat16)
            swapped = jnp.where(low, third, second)
            for i, part in enumerate((first, swapped)):
                h = 2 * p + i
                query = jnp.concatenate([part.astype(jnp.bfloat16), turned], 1)
                top = None
                for s0, s1, t1 in ((0, 256, 256), (256, 512, 512)):
                    x = jnp.dot(query[s0:s1], kc_ref[h, :, 0:t1], preferred_element_type=jnp.float32)
                    x = x + bias_ref[s0:s1, 0:t1]
                    for t in range(0, t1, 128):
                        y = jnp.max(x[:, t : t + 128].reshape(32, 8, 128), axis=0)
                        top = y if top is None else jnp.maximum(top, y)
                top_ref[h] = top
    spot = lax.broadcasted_iota(jnp.int32, (1, 128), 1)
    out = jnp.zeros((1, 128), jnp.float32)
    for h in range(heads):
        best = jnp.max(jnp.max(top_ref[h], axis=0, keepdims=True), axis=1, keepdims=True)
        out = jnp.where(spot == h, best, out)
    out = out * (1.0 / wire_scale) * HEAD ** (-0.5)
    o_ref[...] = jnp.broadcast_to(out, o_ref.shape)


def local_maxima(q, kv, kw, seg, copies):
    cosine, sine = rope_tables()
    heads = kw.shape[1] // NOPE
    vmem = pl.BlockSpec(memory_space=pltpu.VMEM)
    return pl.pallas_call(
        maxima_kernel,
        out_shape=jax.ShapeDtypeStruct((copies, 128), jnp.float32),
        in_specs=[vmem] * 6,
        out_specs=vmem,
        scratch_shapes=[
            pltpu.VMEM((heads, 256, SEQ), jnp.bfloat16),
            pltpu.VMEM((SEQ, SEQ), jnp.float32),
            pltpu.VMEM((heads, 8, 128), jnp.float32),
        ],
        compiler_params=pltpu.CompilerParams(vmem_limit_bytes=16 << 20),
    )(q, kv, kw, seg, jnp.asarray(cosine), jnp.asarray(sine))


def top_kernel(all_ref, top_ref):
    best = all_ref[0:8]
    for i in range(8, all_ref.shape[0], 8):
        best = jnp.maximum(best, all_ref[i : i + 8])
    top_ref[...] = jnp.broadcast_to(jnp.max(best, axis=0, keepdims=True), top_ref.shape)


def top_rows(everything, layers):
    vmem = pl.BlockSpec(memory_space=pltpu.VMEM)
    return pl.pallas_call(
        top_kernel,
        out_shape=jax.ShapeDtypeStruct((layers, 128), jnp.float32),
        in_specs=[vmem],
        out_specs=vmem,
        compiler_params=pltpu.CompilerParams(vmem_limit_bytes=8 << 20),
    )(everything)


def finish_kernel(top_ref, wq_ref, wk_ref, sq_hbm, sk_hbm, sq_ref, sk_ref, sems):
    heads = wk_ref.shape[1] // NOPE
    factor = clip_threshold / jnp.maximum(top_ref[0:1, :], clip_threshold)
    root = jnp.sqrt(factor)
    column = lax.broadcasted_iota(jnp.int32, (1, wq_ref.shape[1]), 1)
    q_scale = jnp.zeros((1, wq_ref.shape[1]), jnp.float32)
    for h in range(heads):
        q_scale = jnp.where(column >= h * HEAD, root[:, h : h + 1], q_scale)
        q_scale = jnp.where(column >= h * HEAD + NOPE, factor[:, h : h + 1], q_scale)
    k_scale = jnp.concatenate([jnp.broadcast_to(root[:, h : h + 1], (1, NOPE)) for h in range(heads)], 1)

    def write(part):
        rows = pl.ds(pl.multiple_of(part * PART, PART), PART)
        return pltpu.make_async_copy(sk_ref.at[rows], sk_hbm.at[rows], sems.at[part])

    def scale(part, carry):
        rows = pl.ds(pl.multiple_of(part * PART, PART), PART)
        sk_ref[rows] = (wk_ref[rows].astype(jnp.float32) * k_scale).astype(jnp.bfloat16)

        @pl.when(part > 0)
        def _():
            write(part - 1).start()

        return carry

    parts = wk_ref.shape[0] // PART
    lax.fori_loop(0, parts, scale, 0)
    sq_ref[...] = (wq_ref[...].astype(jnp.float32) * q_scale).astype(jnp.bfloat16)
    write(parts - 1).start()
    last = pltpu.make_async_copy(sq_ref, sq_hbm, sems.at[parts])
    last.start()
    for part in range(parts):
        write(part).wait()
    last.wait()


def finish(top, wq, wk):
    vmem = pl.BlockSpec(memory_space=pltpu.VMEM)
    away = pl.BlockSpec(memory_space=pl.ANY)
    return pl.pallas_call(
        finish_kernel,
        out_shape=(
            jax.ShapeDtypeStruct(wq.shape, jnp.bfloat16),
            jax.ShapeDtypeStruct(wk.shape, jnp.bfloat16),
        ),
        in_specs=[vmem, vmem, vmem],
        out_specs=(away, away),
        scratch_shapes=[
            pltpu.VMEM(wq.shape, jnp.bfloat16),
            pltpu.VMEM(wk.shape, jnp.bfloat16),
            pltpu.SemaphoreType.DMA((wk.shape[0] // PART + 1,)),
        ],
        cost_estimate=pl.CostEstimate(flops=4_000_000, bytes_accessed=2_500_000, transcendentals=0),
        compiler_params=pltpu.CompilerParams(vmem_limit_bytes=8 << 20),
    )(top, wq, wk)


def per_device(q_latent, kv_latent, segment_ids, q_weight, k_weight):
    layers = lax.axis_size("section")
    copies = lax.axis_size("dp")
    heads = k_weight.shape[2] // NOPE
    sent = (q_weight[0].astype(jnp.float32) * wire_scale).astype(jnp.float16)
    gathered = lax.all_gather(sent, "dp", axis=0, tiled=True).astype(jnp.bfloat16)
    kv = jnp.swapaxes(kv_latent[0], 0, 1)
    q = jnp.dot(q_latent[0], gathered, preferred_element_type=jnp.float32)
    own = local_maxima(q, kv, k_weight[0], segment_ids.reshape(1, -1), copies)
    everything = lax.all_to_all(own.reshape(copies, 1, 128), "dp", 0, 0, tiled=True)
    top = top_rows(everything.reshape(copies, 128), layers)
    table = lax.all_to_all(top.reshape(layers, 1, 128), "section", 0, 0, tiled=True)
    scaled_q, scaled_k = finish(top, q_weight[0], k_weight[0])
    return table[:, 0, :heads] / clip_threshold, scaled_q[None], scaled_k[None]


def solution(mesh):
    return jax.shard_map(
        per_device,
        mesh=mesh,
        in_specs=(
            P("section", "dp", None),
            P("section", "dp", None),
            P("dp"),
            P("section", "dp", "head"),
            P("section", None, "head"),
        ),
        out_specs=(P(None, "head"), P("section", "dp", "head"), P("section", None, "head")),
        check_vma=False,
    )
```

```python
import jax
import jax.numpy as jnp
import numpy as np
from jax import lax
from jax.experimental import pallas as pl
from jax.experimental.pallas import tpu as pltpu
from jax.sharding import PartitionSpec as P

D_Q = 1536
D_KV = 512
NOPE = 128
ROPE = 64
HEAD = NOPE + ROPE
SEQ = 512

clip_threshold = 100.0
rope_base = 50000.0
wire_scale = 512.0
masked = -1e30
PART = 64


def rope_tables():
    half = ROPE // 2
    frequency = np.float32(rope_base) ** (-np.arange(half, dtype=np.float32) / np.float32(half))
    angles = np.arange(SEQ, dtype=np.float32)[:, None] * frequency[None, :].astype(np.float32)
    cosine = np.cos(angles.astype(np.float64)).astype(np.float32)
    sine = np.sin(angles.astype(np.float64)).astype(np.float32)
    return np.tile(cosine, (1, 4)), np.concatenate([-sine, sine, -sine, sine], 1)


def maxima_kernel(q_ref, kv_ref, kw_ref, seg_ref, cos_ref, sin_ref, o_ref, kc_ref, bias_ref, top_ref):
    heads = kw_ref.shape[1] // NOPE
    lane = lax.broadcasted_iota(jnp.int32, (SEQ, 128), 1)
    low = lane < 64
    keys = lax.dot_general(
        kw_ref[...], kv_ref[0:D_KV, :], (((0,), (0,)), ((), ())), preferred_element_type=jnp.float32
    ).astype(jnp.bfloat16)
    shared = kv_ref[D_KV : D_KV + ROPE, :]
    nothing = jnp.zeros_like(shared)
    for h in range(heads):
        upper = keys[h * NOPE : h * NOPE + 64]
        lower = keys[h * NOPE + 64 : (h + 1) * NOPE]
        if h % 2 == 0:
            kc_ref[h] = jnp.concatenate([upper, lower, shared, nothing], 0)
        else:
            kc_ref[h] = jnp.concatenate([lower, upper, nothing, shared], 0)
    row = seg_ref[...].astype(jnp.float32)
    column = jnp.transpose(jnp.broadcast_to(row, (128, SEQ)))
    position = lax.broadcasted_iota(jnp.int32, (SEQ, 128), 0)
    for j in range(SEQ // 128):
        here = slice(j * 128, (j + 1) * 128)
        same = column == jnp.broadcast_to(row[:, here], (SEQ, 128))
        bias_ref[:, here] = jnp.where(same & (lane + j * 128 <= position), 0.0, masked)
    for g in range(heads // 4):
        for p in range(2 * g, 2 * g + 2):
            first = q_ref[:, p * 384 : p * 384 + 128]
            second = q_ref[:, p * 384 + 128 : p * 384 + 256]
            third = q_ref[:, p * 384 + 256 : p * 384 + 384]
            turn = jnp.where(low, second, third)
            partner = jnp.where(lane % 64 < 32, pltpu.roll(turn, 96, 1), pltpu.roll(turn, 32, 1))
            turned = (turn * cos_ref[...] + partner * sin_ref[...]).astype(jnp.bfloat16)
            swapped = jnp.where(low, third, second)
            for i, part in enumerate((first, swapped)):
                h = 2 * p + i
                query = jnp.concatenate([part.astype(jnp.bfloat16), turned], 1)
                top = None
                for s0, s1, t1 in ((0, 256, 256), (256, 512, 512)):
                    x = jnp.dot(query[s0:s1], kc_ref[h, :, 0:t1], preferred_element_type=jnp.float32)
                    x = x + bias_ref[s0:s1, 0:t1]
                    for t in range(0, t1, 128):
                        y = jnp.max(x[:, t : t + 128].reshape(32, 8, 128), axis=0)
                        top = y if top is None else jnp.maximum(top, y)
                top_ref[h] = top
    spot = lax.broadcasted_iota(jnp.int32, (1, 128), 1)
    out = jnp.zeros((1, 128), jnp.float32)
    for h in range(heads):
        best = jnp.max(jnp.max(top_ref[h], axis=0, keepdims=True), axis=1, keepdims=True)
        out = jnp.where(spot == h, best, out)
    out = out * (1.0 / wire_scale) * HEAD ** (-0.5)
    o_ref[...] = jnp.broadcast_to(out, o_ref.shape)


def local_maxima(q, kv, kw, seg, copies):
    cosine, sine = rope_tables()
    heads = kw.shape[1] // NOPE
    vmem = pl.BlockSpec(memory_space=pltpu.VMEM)
    return pl.pallas_call(
        maxima_kernel,
        out_shape=jax.ShapeDtypeStruct((copies, 128), jnp.float32),
        in_specs=[vmem] * 6,
        out_specs=vmem,
        scratch_shapes=[
            pltpu.VMEM((heads, 256, SEQ), jnp.bfloat16),
            pltpu.VMEM((SEQ, SEQ), jnp.float32),
            pltpu.VMEM((heads, 8, 128), jnp.float32),
        ],
        compiler_params=pltpu.CompilerParams(vmem_limit_bytes=16 << 20),
    )(q, kv, kw, seg, jnp.asarray(cosine), jnp.asarray(sine))


def finish_kernel(all_ref, wq_ref, wk_ref, ratio_hbm, sq_hbm, sk_hbm, ratio_ref, sq_ref, sk_ref, sems):
    layers, heads = ratio_ref.shape
    best = all_ref[0:8]
    for i in range(8, all_ref.shape[0], 8):
        best = jnp.maximum(best, all_ref[i : i + 8])
    best = jnp.maximum(best, pltpu.roll(best, 4, 0))
    ratio_ref[...] = best[0:layers, 0:heads] / clip_threshold
    row = lax.broadcasted_iota(jnp.int32, best.shape, 0)
    mine = jnp.where(row % layers == lax.axis_index("section"), best, -jnp.inf)
    own = jnp.max(mine, axis=0, keepdims=True)
    factor = clip_threshold / jnp.maximum(own, clip_threshold)
    root = jnp.sqrt(factor)
    k_scale = jnp.concatenate([jnp.broadcast_to(root[:, h : h + 1], (1, NOPE)) for h in range(heads)], 1)

    def write(part):
        rows = pl.ds(pl.multiple_of(part * PART, PART), PART)
        return pltpu.make_async_copy(sk_ref.at[rows], sk_hbm.at[rows], sems.at[part])

    def scale(part, carry):
        rows = pl.ds(pl.multiple_of(part * PART, PART), PART)
        sk_ref[rows] = (wk_ref[rows].astype(jnp.float32) * k_scale).astype(jnp.bfloat16)

        @pl.when(part > 0)
        def _():
            write(part - 1).start()

        return carry

    parts = wk_ref.shape[0] // PART
    lax.fori_loop(0, parts, scale, 0)
    column = lax.broadcasted_iota(jnp.int32, (1, wq_ref.shape[1]), 1)
    q_scale = jnp.zeros((1, wq_ref.shape[1]), jnp.float32)
    for h in range(heads):
        q_scale = jnp.where(column >= h * HEAD, root[:, h : h + 1], q_scale)
        q_scale = jnp.where(column >= h * HEAD + NOPE, factor[:, h : h + 1], q_scale)
    sq_ref[...] = (wq_ref[...].astype(jnp.float32) * q_scale).astype(jnp.bfloat16)
    write(parts - 1).start()
    others = [
        pltpu.make_async_copy(ratio_ref, ratio_hbm, sems.at[parts]),
        pltpu.make_async_copy(sq_ref, sq_hbm, sems.at[parts + 1]),
    ]
    for other in others:
        other.start()
    for part in range(parts):
        write(part).wait()
    for other in others:
        other.wait()


def finish(everything, wq, wk, layers):
    heads = wk.shape[1] // NOPE
    vmem = pl.BlockSpec(memory_space=pltpu.VMEM)
    away = pl.BlockSpec(memory_space=pl.ANY)
    return pl.pallas_call(
        finish_kernel,
        out_shape=(
            jax.ShapeDtypeStruct((layers, heads), jnp.float32),
            jax.ShapeDtypeStruct(wq.shape, jnp.bfloat16),
            jax.ShapeDtypeStruct(wk.shape, jnp.bfloat16),
        ),
        in_specs=[vmem, vmem, vmem],
        out_specs=(away, away, away),
        scratch_shapes=[
            pltpu.VMEM((layers, heads), jnp.float32),
            pltpu.VMEM(wq.shape, jnp.bfloat16),
            pltpu.VMEM(wk.shape, jnp.bfloat16),
            pltpu.SemaphoreType.DMA((wk.shape[0] // PART + 2,)),
        ],
        compiler_params=pltpu.CompilerParams(vmem_limit_bytes=8 << 20),
    )(everything, wq, wk)


def per_device(q_latent, kv_latent, segment_ids, q_weight, k_weight):
    layers = lax.axis_size("section")
    copies = lax.axis_size("dp") * layers
    sent = (q_weight[0].astype(jnp.float32) * wire_scale).astype(jnp.float16)
    gathered = lax.all_gather(sent, "dp", axis=0, tiled=True).astype(jnp.bfloat16)
    kv = jnp.swapaxes(kv_latent[0], 0, 1)
    q = jnp.dot(q_latent[0], gathered, preferred_element_type=jnp.float32)
    own = local_maxima(q, kv, k_weight[0], segment_ids.reshape(1, -1), copies)
    everything = lax.all_to_all(own.reshape(copies, 1, 128), ("dp", "section"), 0, 0, tiled=True)
    ratio, scaled_q, scaled_k = finish(everything.reshape(copies, 128), q_weight[0], k_weight[0], layers)
    return ratio, scaled_q[None], scaled_k[None]


def solution(mesh):
    return jax.shard_map(
        per_device,
        mesh=mesh,
        in_specs=(
            P("section", "dp", None),
            P("section", "dp", None),
            P("dp"),
            P("section", "dp", "head"),
            P("section", None, "head"),
        ),
        out_specs=(P(None, "head"), P("section", "dp", "head"), P("section", None, "head")),
        check_vma=False,
    )
```

```python
import jax
import jax.numpy as jnp
import numpy as np
from jax import lax
from jax.experimental import pallas as pl
from jax.experimental.pallas import tpu as pltpu
from jax.sharding import PartitionSpec as P

D_Q = 1536
D_KV = 512
NOPE = 128
ROPE = 64
HEAD = NOPE + ROPE
SEQ = 512

clip_threshold = 100.0
rope_base = 50000.0
wire_scale = 512.0
masked = -1e30
PART = 128


def rope_tables():
    half = ROPE // 2
    frequency = np.float32(rope_base) ** (-np.arange(half, dtype=np.float32) / np.float32(half))
    angles = np.arange(SEQ, dtype=np.float32)[:, None] * frequency[None, :].astype(np.float32)
    cosine = np.cos(angles.astype(np.float64)).astype(np.float32)
    sine = np.sin(angles.astype(np.float64)).astype(np.float32)
    return np.tile(cosine, (1, 4)), np.concatenate([-sine, sine, -sine, sine], 1)


def maxima_kernel(q_ref, kv_ref, kw_ref, seg_ref, cos_ref, sin_ref, o_ref, kc_ref, bias_ref, top_ref):
    heads = kw_ref.shape[1] // NOPE
    lane = lax.broadcasted_iota(jnp.int32, (SEQ, 128), 1)
    low = lane < 64
    keys = lax.dot_general(
        kw_ref[...], kv_ref[0:D_KV, :], (((0,), (0,)), ((), ())), preferred_element_type=jnp.float32
    ).astype(jnp.bfloat16)
    shared = kv_ref[D_KV : D_KV + ROPE, :]
    nothing = jnp.zeros_like(shared)
    for h in range(heads):
        upper = keys[h * NOPE : h * NOPE + 64]
        lower = keys[h * NOPE + 64 : (h + 1) * NOPE]
        if h % 2 == 0:
            kc_ref[h] = jnp.concatenate([upper, lower, shared, nothing], 0)
        else:
            kc_ref[h] = jnp.concatenate([lower, upper, nothing, shared], 0)
    row = seg_ref[...].astype(jnp.float32)
    column = jnp.transpose(jnp.broadcast_to(row, (128, SEQ)))
    position = lax.broadcasted_iota(jnp.int32, (SEQ, 128), 0)
    for j in range(SEQ // 128):
        here = slice(j * 128, (j + 1) * 128)
        on = slice(j * 128, (j + 1) * 128)
        tail = slice((j + 1) * 128, SEQ)
        same = column[on] == jnp.broadcast_to(row[:, here], (128, 128))
        bias_ref[on, here] = jnp.where(same & (lane[on] <= position[0:128]), 0.0, masked)
        if j < 3:
            same = column[tail] == jnp.broadcast_to(row[:, here], (SEQ - (j + 1) * 128, 128))
            bias_ref[tail, here] = jnp.where(same, 0.0, masked)
        if j % 2 == 1:
            bias_ref[(j - 1) * 128 : j * 128, here] = jnp.full((128, 128), masked, jnp.float32)
    for g in range(heads // 4):
        for p in range(2 * g, 2 * g + 2):
            first = q_ref[:, p * 384 : p * 384 + 128]
            second = q_ref[:, p * 384 + 128 : p * 384 + 256]
            third = q_ref[:, p * 384 + 256 : p * 384 + 384]
            turn = jnp.where(low, second, third)
            partner = jnp.where(lane % 64 < 32, pltpu.roll(turn, 96, 1), pltpu.roll(turn, 32, 1))
            turned = (turn * cos_ref[...] + partner * sin_ref[...]).astype(jnp.bfloat16)
            swapped = jnp.where(low, third, second)
            for i, part in enumerate((first, swapped)):
                h = 2 * p + i
                query = jnp.concatenate([part.astype(jnp.bfloat16), turned], 1)
                top = None
                for s0, s1, t1 in ((0, 256, 256), (256, 512, 512)):
                    x = jnp.dot(query[s0:s1], kc_ref[h, :, 0:t1], preferred_element_type=jnp.float32)
                    x = x + bias_ref[s0:s1, 0:t1]
                    for t in range(0, t1, 128):
                        y = jnp.max(x[:, t : t + 128].reshape(32, 8, 128), axis=0)
                        top = y if top is None else jnp.maximum(top, y)
                top_ref[h] = top
    spot = lax.broadcasted_iota(jnp.int32, (1, 128), 1)
    out = jnp.zeros((1, 128), jnp.float32)
    for h in range(heads):
        best = jnp.max(jnp.max(top_ref[h], axis=0, keepdims=True), axis=1, keepdims=True)
        out = jnp.where(spot == h, best, out)
    out = out * (1.0 / wire_scale) * HEAD ** (-0.5)
    o_ref[...] = jnp.broadcast_to(out, o_ref.shape)


def local_maxima(q, kv, kw, seg, copies):
    cosine, sine = rope_tables()
    heads = kw.shape[1] // NOPE
    vmem = pl.BlockSpec(memory_space=pltpu.VMEM)
    return pl.pallas_call(
        maxima_kernel,
        out_shape=jax.ShapeDtypeStruct((copies, 128), jnp.float32),
        in_specs=[vmem] * 6,
        out_specs=vmem,
        scratch_shapes=[
            pltpu.VMEM((heads, 256, SEQ), jnp.bfloat16),
            pltpu.VMEM((SEQ, SEQ), jnp.float32),
            pltpu.VMEM((heads, 8, 128), jnp.float32),
        ],
        compiler_params=pltpu.CompilerParams(vmem_limit_bytes=16 << 20),
    )(q, kv, kw, seg, jnp.asarray(cosine), jnp.asarray(sine))


def finish_kernel(all_ref, wq_ref, wk_ref, ratio_hbm, sq_hbm, sk_hbm, ratio_ref, sq_ref, sk_ref, sems):
    layers, heads = ratio_ref.shape
    best = all_ref[0:8]
    for i in range(8, all_ref.shape[0], 8):
        best = jnp.maximum(best, all_ref[i : i + 8])
    best = jnp.maximum(best, pltpu.roll(best, 4, 0))
    ratio_ref[...] = best[0:layers, 0:heads] / clip_threshold
    row = lax.broadcasted_iota(jnp.int32, best.shape, 0)
    mine = jnp.where(row % layers == lax.axis_index("section"), best, -jnp.inf)
    own = jnp.max(mine, axis=0, keepdims=True)
    factor = clip_threshold / jnp.maximum(own, clip_threshold)
    root = jnp.sqrt(factor)
    column = lax.broadcasted_iota(jnp.int32, (1, wq_ref.shape[1]), 1)
    q_scale = jnp.zeros((1, wq_ref.shape[1]), jnp.float32)
    for h in range(heads):
        q_scale = jnp.where(column >= h * HEAD, root[:, h : h + 1], q_scale)
        q_scale = jnp.where(column >= h * HEAD + NOPE, factor[:, h : h + 1], q_scale)
    k_scale = jnp.concatenate([jnp.broadcast_to(root[:, h : h + 1], (1, NOPE)) for h in range(heads)], 1)

    def write(part):
        rows = pl.ds(pl.multiple_of(part * PART, PART), PART)
        return pltpu.make_async_copy(sk_ref.at[rows], sk_hbm.at[rows], sems.at[part])

    def scale(part, carry):
        rows = pl.ds(pl.multiple_of(part * PART, PART), PART)
        sk_ref[rows] = (wk_ref[rows].astype(jnp.float32) * k_scale).astype(jnp.bfloat16)

        @pl.when(part > 0)
        def _():
            write(part - 1).start()

        return carry

    parts = wk_ref.shape[0] // PART
    lax.fori_loop(0, parts, scale, 0)
    sq_ref[...] = (wq_ref[...].astype(jnp.float32) * q_scale).astype(jnp.bfloat16)
    write(parts - 1).start()
    others = [
        pltpu.make_async_copy(ratio_ref, ratio_hbm, sems.at[parts]),
        pltpu.make_async_copy(sq_ref, sq_hbm, sems.at[parts + 1]),
    ]
    for other in others:
        other.start()
    for part in range(parts):
        write(part).wait()
    for other in others:
        other.wait()


def finish(everything, wq, wk, layers):
    heads = wk.shape[1] // NOPE
    vmem = pl.BlockSpec(memory_space=pltpu.VMEM)
    away = pl.BlockSpec(memory_space=pl.ANY)
    return pl.pallas_call(
        finish_kernel,
        out_shape=(
            jax.ShapeDtypeStruct((layers, heads), jnp.float32),
            jax.ShapeDtypeStruct(wq.shape, jnp.bfloat16),
            jax.ShapeDtypeStruct(wk.shape, jnp.bfloat16),
        ),
        in_specs=[vmem, vmem, vmem],
        out_specs=(away, away, away),
        scratch_shapes=[
            pltpu.VMEM((layers, heads), jnp.float32),
            pltpu.VMEM(wq.shape, jnp.bfloat16),
            pltpu.VMEM(wk.shape, jnp.bfloat16),
            pltpu.SemaphoreType.DMA((wk.shape[0] // PART + 2,)),
        ],
        compiler_params=pltpu.CompilerParams(vmem_limit_bytes=8 << 20),
    )(everything, wq, wk)


def per_device(q_latent, kv_latent, segment_ids, q_weight, k_weight):
    layers = lax.axis_size("section")
    copies = lax.axis_size("dp") * layers
    sent = (q_weight[0].astype(jnp.float32) * wire_scale).astype(jnp.float16)
    gathered = lax.all_gather(sent, "dp", axis=0, tiled=True).astype(jnp.bfloat16)
    kv = jnp.swapaxes(kv_latent[0], 0, 1)
    q = jnp.dot(q_latent[0], gathered, preferred_element_type=jnp.float32)
    own = local_maxima(q, kv, k_weight[0], segment_ids.reshape(1, -1), copies)
    everything = lax.all_to_all(own.reshape(copies, 1, 128), ("dp", "section"), 0, 0, tiled=True)
    ratio, scaled_q, scaled_k = finish(everything.reshape(copies, 128), q_weight[0], k_weight[0], layers)
    return ratio, scaled_q[None], scaled_k[None]


def solution(mesh):
    return jax.shard_map(
        per_device,
        mesh=mesh,
        in_specs=(
            P("section", "dp", None),
            P("section", "dp", None),
            P("dp"),
            P("section", "dp", "head"),
            P("section", None, "head"),
        ),
        out_specs=(P(None, "head"), P("section", "dp", "head"), P("section", None, "head")),
        check_vma=False,
    )
```
